32 devices in a mesh: rep: 4 (over x, y), dp: 8 (over z, core).
Axes of the slice: x: 2, y: 2, z: 4, core: 2. Of those that a mesh axis runs over, the one named last changes fastest.
Arguments:
- x: bfloat16 [32, 2048, 512], P(('rep', 'dp')), parts along dimension 0
- dy: bfloat16 [32, 2048, 512], P(('rep', 'dp')), parts along dimension 0
- wq: bfloat16 [2, 512, 1024], P(None, 'dp')
- wk: bfloat16 [2, 512, 512], P(None, 'dp')
- wv: bfloat16 [2, 512, 512], P(None, 'dp')
- wo: bfloat16 [2, 1024, 512], P(None, 'dp')
- w_gate: bfloat16 [2, 512, 1536], P(None, 'dp')
- w_up: bfloat16 [2, 512, 1536], P(None, 'dp')
- w_down: bfloat16 [2, 1536, 512], P(None, 'dp')
- m_wq: float32 [2, 512, 1024], P(None, 'dp')
- m_wk: float32 [2, 512, 512], P(None, 'dp')
- m_wv: float32 [2, 512, 512], P(None, 'dp')
- m_wo: float32 [2, 1024, 512], P(None, 'dp')
- m_w_gate: float32 [2, 512, 1536], P(None, 'dp')
- m_w_up: float32 [2, 512, 1536], P(None, 'dp')
- m_w_down: float32 [2, 1536, 512], P(None, 'dp')
- v_wq: float32 [2, 512, 1024], P(None, 'dp')
- v_wk: float32 [2, 512, 512], P(None, 'dp')
- v_wv: float32 [2, 512, 512], P(None, 'dp')
- v_wo: float32 [2, 1024, 512], P(None, 'dp')
- v_w_gate: float32 [2, 512, 1536], P(None, 'dp')
- v_w_up: float32 [2, 512, 1536], P(None, 'dp')
- v_w_down: float32 [2, 1536, 512], P(None, 'dp')
Outputs:
- output 1: bfloat16 [8, 512, 1024], P('rep', 'dp'), parts along dimension 0
- output 2: bfloat16 [8, 512, 512], P('rep', 'dp'), parts along dimension 0
- output 3: bfloat16 [8, 512, 512], P('rep', 'dp'), parts along dimension 0
- output 4: bfloat16 [8, 1024, 512], P('rep', 'dp'), parts along dimension 0
- output 5: bfloat16 [8, 512, 1536], P('rep', 'dp'), parts along dimension 0
- output 6: bfloat16 [8, 512, 1536], P('rep', 'dp'), parts along dimension 0
- output 7: bfloat16 [8, 1536, 512], P('rep', 'dp'), parts along dimension 0
- output 8: float32 [8, 512, 1024], P('rep', 'dp'), parts along dimension 0
- output 9: float32 [8, 512, 512], P('rep', 'dp'), parts along dimension 0
- output 10: float32 [8, 512, 512], P('rep', 'dp'), parts along dimension 0
- output 11: float32 [8, 1024, 512], P('rep', 'dp'), parts along dimension 0
- output 12: float32 [8, 512, 1536], P('rep', 'dp'), parts along dimension 0
- output 13: float32 [8, 512, 1536], P('rep', 'dp'), parts along dimension 0
- output 14: float32 [8, 1536, 512], P('rep', 'dp'), parts along dimension 0
- output 15: float32 [8, 512, 1024], P('rep', 'dp'), parts along dimension 0
- output 16: float32 [8, 512, 512], P('rep', 'dp'), parts along dimension 0
- output 17: float32 [8, 512, 512], P('rep', 'dp'), parts along dimension 0
- output 18: float32 [8, 1024, 512], P('rep', 'dp'), parts along dimension 0
- output 19: float32 [8, 512, 1536], P('rep', 'dp'), parts along dimension 0
- output 20: float32 [8, 512, 1536], P('rep', 'dp'), parts along dimension 0
- output 21: float32 [8, 1536, 512], P('rep', 'dp'), parts along dimension 0
There are 4 independent parts. The reference program is written for one: setup_inputs(seed, part) draws one part's arguments, and reference() takes and returns one part's arrays. A program takes and returns all parts, laid end to end along the dimension named above; an argument that names none is the same for every part.
All inputs are finite; a program needn't handle non-finite values.
Results may differ from the reference program's by a relative error of at most 0.024.
Values are sent between devices in bfloat16 or wider.
A program may use at most 2 GiB of HBM per device.

```python
import jax
import jax.numpy as jnp
from jax import lax

SEQUENCES = 8
TOKENS = 2048
D = 512
HEADS = 8
KV_HEADS = 4
HEAD = 128
FF = 1536
LAYERS = 2
THETA = 10000
NAMES = ("wq", "wk", "wv", "wo", "w_gate", "w_up", "w_down")
SHAPES = {
    "wq": (LAYERS, D, HEADS * HEAD),
    "wk": (LAYERS, D, KV_HEADS * HEAD),
    "wv": (LAYERS, D, KV_HEADS * HEAD),
    "wo": (LAYERS, HEADS * HEAD, D),
    "w_gate": (LAYERS, D, FF),
    "w_up": (LAYERS, D, FF),
    "w_down": (LAYERS, FF, D),
}


def bump(key, n, height):
    away = (jnp.arange(n, dtype=jnp.int32) - jax.random.randint(key, (), 0, n, jnp.int32)) % n
    return jnp.where(away < n // 8, height, 1.0)


def together(key, own, strength):
    shared = jax.random.normal(key, own.shape[1:], jnp.float32)
    return (own + strength * shared) * lax.rsqrt(1 + strength * strength)


def setup_inputs(seed: int = 0, part: int = 0) -> dict:
    kx, kdy, ka, kb, kz, kf, kh, kl, *keys = jax.random.split(jax.random.key(seed), 8 + 3 * len(NAMES))
    kx, kdy, ka, kb = (jax.random.fold_in(k, part) for k in (kx, kdy, ka, kb))
    kw, km, kv = (keys[i::3] for i in range(3))
    shape = (SEQUENCES, TOKENS, D)
    much_x, much_dy = jax.random.uniform(kz, (2,), jnp.float32, 0.0, 1.0)
    loud = 2.0 ** jax.random.uniform(jax.random.fold_in(kz, 1), (), jnp.float32, -1.0, 2.0)
    layers = 2.0 ** jax.random.uniform(kl, (LAYERS, 1, 1), jnp.float32, -1.0, 1.0)
    times = {"wq": 1.0, "wk": 1.0, "wv": 2.0, "wo": layers, "w_gate": 1.0, "w_up": bump(kh, FF, 4.0), "w_down": layers}
    x = together(ka, jax.random.normal(kx, shape, jnp.float32), much_x) * bump(kf, D, 4.0)
    dy = together(kb, jax.random.normal(kdy, shape, jnp.float32), much_dy)
    drawn = {"x": x.astype(jnp.bfloat16), "dy": (loud * dy * (SEQUENCES * TOKENS) ** -0.5).astype(jnp.bfloat16)}
    for key, name in zip(kw, NAMES, strict=True):
        drawn[name] = (jax.random.normal(key, SHAPES[name], jnp.float32) * SHAPES[name][1] ** -0.5 * times[name]).astype(jnp.bfloat16)
    for key, name in zip(km, NAMES, strict=True):
        drawn[f"m_{name}"] = 0.1 * jax.random.normal(key, SHAPES[name], jnp.float32)
    for key, name in zip(kv, NAMES, strict=True):
        drawn[f"v_{name}"] = loud * loud * jax.random.uniform(key, SHAPES[name], jnp.float32, 0.2, 0.6)
    return drawn


def matmul(a, w):
    return jnp.dot(a, w, preferred_element_type=jnp.float32).astype(jnp.bfloat16)


def normed(h):
    wide = h.astype(jnp.float32)
    scale = lax.rsqrt(jnp.mean(wide**2, -1, keepdims=True) + 1e-6)
    return (wide * scale).astype(jnp.bfloat16)


def turned(t, theta):
    half = t.shape[-1] // 2
    angle = jnp.arange(t.shape[0], dtype=jnp.float32)[:, None] * theta ** (-jnp.arange(half, dtype=jnp.float32) / half)
    cos, sin = jnp.cos(angle)[:, None], jnp.sin(angle)[:, None]
    a, b = t[..., :half].astype(jnp.float32), t[..., half:].astype(jnp.float32)
    return jnp.concatenate([a * cos - b * sin, b * cos + a * sin], -1).astype(jnp.bfloat16)


def seen_by(q, k, v):
    tokens, kv = q.shape[0], k.shape[1]
    q = q.reshape(tokens, kv, -1, q.shape[-1])
    scores = jnp.einsum("tgsd,ugd->gstu", q.astype(jnp.float32), k.astype(jnp.float32)) * q.shape[-1] ** -0.5
    place = jnp.arange(tokens)
    weights = jax.nn.softmax(jnp.where(place[:, None] >= place, scores, -jnp.inf), -1).astype(jnp.bfloat16)
    return jnp.einsum("gstu,ugd->tgsd", weights.astype(jnp.float32), v.astype(jnp.float32)).astype(jnp.bfloat16).reshape(tokens, -1)


def layer(h, w):
    a = normed(h)
    q, k = (turned(matmul(a, w[name]).reshape(h.shape[0], -1, HEAD), THETA) for name in ("wq", "wk"))
    h = h + matmul(seen_by(q, k, matmul(a, w["wv"]).reshape(h.shape[0], -1, HEAD)), w["wo"])
    b = normed(h)
    gate = jnp.dot(b, w["w_gate"], preferred_element_type=jnp.float32)
    up = jnp.dot(b, w["w_up"], preferred_element_type=jnp.float32)
    return h + matmul((jax.nn.silu(gate) * up).astype(jnp.bfloat16), w["w_down"])


def adamw(w, m, v, g):
    m = 0.9 * m + 0.1 * g
    v = 0.95 * v + 0.05 * g * g
    step = m * lax.rsqrt(v + 1e-8) + 0.1 * w
    return (w - 0.02 * step).astype(jnp.bfloat16), m, v


def stack(weights, h):
    return lax.scan(lambda h, w: (layer(h, w), None), h, weights)[0]


def reference(x, dy, wq, wk, wv, wo, w_gate, w_up, w_down, m_wq, m_wk, m_wv, m_wo, m_w_gate, m_w_up, m_w_down, v_wq, v_wk, v_wv, v_wo, v_w_gate, v_w_up, v_w_down):
    weights = dict(zip(NAMES, (wq, wk, wv, wo, w_gate, w_up, w_down), strict=True))

    def take(so_far, sequence):
        h, by_y = sequence
        _, back = jax.vjp(stack, weights, h)
        by_weights, by_h = back(by_y)
        return jax.tree.map(lambda total, term: total + term.astype(jnp.float32), so_far, by_weights), by_h

    none_yet = {name: jnp.zeros(w.shape, jnp.float32) for name, w in weights.items()}
    by_weights, by_x = lax.scan(take, none_yet, (x, dy))
    gradients = [by_weights[name].astype(jnp.bfloat16).astype(jnp.float32) for name in NAMES]
    first = (m_wq, m_wk, m_wv, m_wo, m_w_gate, m_w_up, m_w_down)
    second = (v_wq, v_wk, v_wv, v_wo, v_w_gate, v_w_up, v_w_down)
    new = [adamw(weights[name].astype(jnp.float32), m, v, g) for name, m, v, g in zip(NAMES, first, second, gradients, strict=True)]
    return tuple(one[which] for which in range(3) for one in new)
```

```python
import functools

import jax
import jax.numpy as jnp
from jax import lax
from jax.experimental import pallas as pl
from jax.experimental.pallas import tpu as pltpu
from jax.sharding import PartitionSpec as P

HEAD = 128
THETA = 10000
D = 512
BF16, F32 = jnp.bfloat16, jnp.float32
ROOM = 63 * 2**20
NEG = -1e30
HIDDEN = 2 * NEG
SCALE = HEAD**-0.5
E = SCALE * 1.4426950408889634


def _dot(a, b, ca, cb):
    return lax.dot_general(a, b, (((ca,), (cb,)), ((), ())), preferred_element_type=F32)


def visible(keys, wide, at):
    return lax.broadcasted_iota(jnp.int32, (keys, wide), 1) + at >= lax.broadcasted_iota(jnp.int32, (keys, wide), 0)


def _forward(q_ref, k_ref, v_ref, o_ref, lse_ref, top_s, mix_s, *, b, wide):
    heads, g = q_ref.shape[0], q_ref.shape[1]
    iq = pl.program_id(1)
    strips = [(i, n, at) for i in range(heads) for n in range(g) for at in range(0, b, wide)]
    top_s[...] = jnp.full(top_s.shape, NEG, F32)
    mix_s[...] = jnp.zeros(mix_s.shape, F32)

    def block(j, diagonal):
        start = pl.multiple_of(j * b, b)
        many = [at + wide if diagonal else b for _, _, at in strips]
        scores = [_dot(k_ref[i, pl.ds(start, m), :], q_ref[i, n, at : at + wide, :], 1, 1) for (i, n, at), m in zip(strips, many)]
        weights, keeps = [], []
        for (i, n, at), m, s in zip(strips, many, scores):
            if diagonal:
                s = jnp.where(visible(m, wide, at), s, HIDDEN)
            here = pl.ds(n * b + at, wide)
            old = top_s[i : i + 1, here]
            top = jnp.maximum(old, s.max(axis=0, keepdims=True))
            top_s[i : i + 1, here] = top
            weights.append(jnp.exp2((s - top) * E).astype(BF16))
            keeps.append(jnp.exp2((old - top) * E))
        for (i, n, at), m, p, keep in zip(strips, many, weights, keeps):
            values = jnp.concatenate([v_ref[i, pl.ds(start, m), :].T, jnp.ones((8, m), BF16)], axis=0)
            here = pl.ds(n * b + at, wide)
            mix_s[i, :, here] = mix_s[i, :, here] * keep + _dot(values, p, 1, 0)

    lax.fori_loop(0, iq, lambda j, _: block(j, False), None)
    block(iq, True)
    for i in range(heads):
        total = mix_s[i, HEAD : HEAD + 1, :]
        out = (mix_s[i, :HEAD, :] * (1 / total)).T.astype(BF16)
        lse = top_s[i : i + 1, :] * SCALE + jnp.log(total)
        for n in range(g):
            o_ref[i, n] = out[n * b : (n + 1) * b]
            lse_ref[i, n : n + 1, :] = lse[:, n * b : (n + 1) * b]


def _cost(q, k, width):
    return pl.CostEstimate(flops=q.size // HEAD * k.shape[1] * width * HEAD, transcendentals=0, bytes_accessed=4 * (q.size + k.size))


def attend(q, k, v, heads=2, b=1024, wide=256):
    kv, g, t, _ = q.shape
    queries = pl.BlockSpec((heads, g, b, HEAD), lambda ih, iq: (ih, 0, iq, 0))
    keys = pl.BlockSpec((heads, t, HEAD), lambda ih, iq: (ih, 0, 0))
    stats = pl.BlockSpec((heads, g, b), lambda ih, iq: (ih, 0, iq))
    return pl.pallas_call(
        functools.partial(_forward, b=b, wide=wide),
        grid=(kv // heads, t // b),
        in_specs=[queries, keys, keys],
        out_specs=[queries, stats],
        out_shape=[jax.ShapeDtypeStruct(q.shape, BF16), jax.ShapeDtypeStruct((kv, g, t), F32)],
        scratch_shapes=[pltpu.VMEM((heads, g * b), F32), pltpu.VMEM((heads, HEAD + 8, g * b), F32)],
        compiler_params=pltpu.CompilerParams(dimension_semantics=("arbitrary", "arbitrary"), vmem_limit_bytes=ROOM),
        cost_estimate=_cost(q, k, 2),
    )(q, k, v)


def _backward(q_ref, k_ref, v_ref, do_ref, lse_ref, delta_ref, dq_ref, dk_ref, dv_ref, dq_s, dk_s, dv_s, *, b, wide):
    heads, g = q_ref.shape[0], q_ref.shape[1]
    iq = pl.program_id(1)
    strips = [(i, n, at) for i in range(heads) for n in range(g) for at in range(0, b, wide)]

    @pl.when(iq == 0)
    def _():
        dk_s[...] = jnp.zeros_like(dk_s)
        dv_s[...] = jnp.zeros_like(dv_s)

    dq_s[...] = jnp.zeros_like(dq_s)

    def block(j, diagonal):
        start = pl.multiple_of(j * b, b)
        many = [at + wide if diagonal else b for _, _, at in strips]
        qs = [q_ref[i, n, at : at + wide, :] for i, n, at in strips]
        dos = [do_ref[i, n, at : at + wide, :] for i, n, at in strips]
        scores = [_dot(k_ref[i, pl.ds(start, m), :], x, 1, 1) for (i, _, _), m, x in zip(strips, many, qs)]
        dps = [_dot(v_ref[i, pl.ds(start, m), :], x, 1, 1) for (i, _, _), m, x in zip(strips, many, dos)]
        for x, (i, n, at) in enumerate(strips):
            here, m = pl.ds(start, many[x]), many[x]
            p = jnp.exp2(scores[x] * E - lse_ref[i, n : n + 1, at : at + wide] * (E / SCALE))
            if diagonal:
                p = jnp.where(visible(m, wide, at), p, 0.0)
            ds = (p * (dps[x] - delta_ref[i, n : n + 1, at : at + wide])).astype(BF16)
            dv_s[i, here, :] += _dot(p.astype(BF16), dos[x], 1, 0)
            dk_s[i, here, :] += _dot(ds, qs[x], 1, 0)
            dq_s[i, :, pl.ds(n * b + at, wide)] += _dot(k_ref[i, here, :].T, ds, 1, 0)

    lax.fori_loop(0, iq, lambda j, _: block(j, False), None)
    block(iq, True)
    for i in range(heads):
        dq = (dq_s[i] * SCALE).T.astype(BF16)
        for n in range(g):
            dq_ref[i, n] = dq[n * b : (n + 1) * b]

    @pl.when(iq == pl.num_programs(1) - 1)
    def _():
        dk_ref[...] = (dk_s[...] * SCALE).astype(BF16)
        dv_ref[...] = dv_s[...].astype(BF16)


def attend_back(q, k, v, do, lse, delta, heads=1, b=1024, wide=256):
    kv, g, t, _ = q.shape
    queries = pl.BlockSpec((heads, g, b, HEAD), lambda ih, iq: (ih, 0, iq, 0))
    keys = pl.BlockSpec((heads, t, HEAD), lambda ih, iq: (ih, 0, 0))
    stats = pl.BlockSpec((heads, g, b), lambda ih, iq: (ih, 0, iq))
    return pl.pallas_call(
        functools.partial(_backward, b=b, wide=wide),
        grid=(kv // heads, t // b),
        in_specs=[queries, keys, keys, queries, stats, stats],
        out_specs=[queries, keys, keys],
        out_shape=[jax.ShapeDtypeStruct(q.shape, BF16), jax.ShapeDtypeStruct(k.shape, BF16), jax.ShapeDtypeStruct(k.shape, BF16)],
        scratch_shapes=[pltpu.VMEM((heads, HEAD, g * b), F32), pltpu.VMEM((heads, t, HEAD), F32), pltpu.VMEM((heads, t, HEAD), F32)],
        compiler_params=pltpu.CompilerParams(dimension_semantics=("arbitrary", "arbitrary"), vmem_limit_bytes=ROOM),
        cost_estimate=_cost(q, k, 5),
    )(q, k, v, do, lse, delta)


def kernel_call(body, steps, ins, outs, scratch, flops, args):
    moved = sum(a.size * a.dtype.itemsize for a in args) + sum(o.size * o.dtype.itemsize for _, o in outs)
    return pl.pallas_call(
        body,
        grid=(steps,),
        in_specs=ins,
        out_specs=[spec for spec, _ in outs],
        out_shape=[o for _, o in outs],
        scratch_shapes=scratch,
        compiler_params=pltpu.CompilerParams(dimension_semantics=("arbitrary",), vmem_limit_bytes=ROOM),
        cost_estimate=pl.CostEstimate(flops=flops, bytes_accessed=moved, transcendentals=0),
    )(*args)


def shape(s, dtype=BF16):
    return jax.ShapeDtypeStruct(s, dtype)


def tile(*block):
    return pl.BlockSpec(block, lambda i: (0,) * (len(block) - 2) + (i, 0))


def pieces(w):
    array, first, many = w
    one = lambda n: pl.BlockSpec((8, 1, 64, D), lambda i: (0, n, 0, 0), pipeline_mode=pl.Buffered(1))
    return [one(first + n) for n in range(many)], [array] * many


def grads(many):
    return pl.BlockSpec((8, many, 64, D), lambda i: (0, 0, 0, 0), pipeline_mode=pl.Buffered(1)), shape((8, many, 64, D))


def unit(wide):
    return lax.rsqrt(jnp.mean(wide * wide, -1, keepdims=True) + 1e-6)


def unit_back(wide, scale, g):
    return scale * g - wide * (scale * scale * scale * jnp.mean(g * wide, -1, keepdims=True))


def square(w, n):
    return w[n][...].reshape(D, D)


def rows_o(w, m):
    return jnp.concatenate([w[k % 2][k // 2, 0] for k in range(8 * m, 8 * m + 8)], axis=0)


def rows_down(w, n):
    return jnp.concatenate([w[8 + k % 3][k // 3, 0] for k in range(8 * n, 8 * n + 8)], axis=0)


def tables(tokens):
    half = HEAD // 2
    angle = jnp.arange(tokens, dtype=F32)[:, None] * THETA ** (-jnp.arange(half, dtype=F32) / half)
    cos, sin = jnp.cos(angle), jnp.sin(angle)
    return jnp.concatenate([cos, cos], -1), jnp.concatenate([-sin, sin], -1)


def _qkv(h_ref, cos_ref, sin_ref, *refs):
    w, outs = refs[:4], refs[4:]
    wide = h_ref[...].astype(F32)
    a = (wide * unit(wide)).astype(BF16)
    cos, sin = cos_ref[...], sin_ref[...]
    for n in range(4):
        t = _dot(a, square(w, n), 1, 0).astype(BF16)
        for j in range(4):
            one = t[:, j * HEAD : (j + 1) * HEAD]
            if n < 3:
                f = one.astype(F32)
                one = (f * cos + pltpu.roll(f, HEAD // 2, 1) * sin).astype(BF16)
            outs[max(n - 1, 0)][4 * n + j if n < 2 else j] = one


def qkv(h, cos, sin, w, bt=512):
    t = h.shape[0]
    specs, args = pieces(w)
    outs = [(tile(n, bt, HEAD), shape((n, t, HEAD))) for n in (8, 4, 4)]
    return kernel_call(_qkv, t // bt, [tile(bt, D), tile(bt, HEAD), tile(bt, HEAD)] + specs, outs, [], 2 * t * D * 2048, [h, cos, sin] + args)


def silu_parts(g):
    s = 1 / (1 + jnp.exp(-g))
    return s, g * s


def joined(h, o, w):
    halves = [jnp.concatenate([o[4 * m + j] for j in range(4)], axis=1) for m in range(2)]
    x = _dot(halves[0], rows_o(w, 0), 1, 0) + _dot(halves[1], rows_o(w, 1), 1, 0)
    return (h.astype(F32) + x.astype(BF16).astype(F32)).astype(BF16)


def _mlp(h_ref, o_ref, *refs):
    w, (mid_ref, y_ref) = refs[:11], refs[11:]
    mid = joined(h_ref[...], o_ref, w)
    mid_ref[...] = mid
    wide = mid.astype(F32)
    b = (wide * unit(wide)).astype(BF16)
    y = 0.0
    for n in range(3):
        g = _dot(b, square(w, 2 + n), 1, 0)
        u = _dot(b, square(w, 5 + n), 1, 0)
        y += _dot((silu_parts(g)[1] * u).astype(BF16), rows_down(w, n), 1, 0)
    y_ref[...] = (wide + y.astype(BF16).astype(F32)).astype(BF16)


def mlp(h, o, w, bt=512):
    t = h.shape[0]
    specs, args = pieces(w)
    outs = [(tile(bt, D), shape((t, D)))] * 2
    return kernel_call(_mlp, t // bt, [tile(bt, D), tile(8, bt, HEAD)] + specs, outs, [], 2 * t * D * 5632, [h, o] + args)


def _mlp_back(in_ref, dy_ref, o_ref, *refs, last):
    w, (dmid_ref, do_ref, delta_ref, dw_ref, gu_s, down_s, o_s) = refs[:11], refs[11:]
    i = pl.program_id(0)

    @pl.when(i == 0)
    def _():
        gu_s[...] = jnp.zeros_like(gu_s)
        down_s[...] = jnp.zeros_like(down_s)
        o_s[...] = jnp.zeros_like(o_s)

    wide = (joined(in_ref[...], o_ref, w) if last else in_ref[...]).astype(F32)
    scale = unit(wide)
    b = (wide * scale).astype(BF16)
    b_t = b.T
    dy = dy_ref[...]
    dy_t = dy.T
    db = 0.0
    for n in range(3):
        g = _dot(b, square(w, 2 + n), 1, 0)
        u = _dot(b, square(w, 5 + n), 1, 0)
        dact = _dot(dy, rows_down(w, n), 1, 1).astype(BF16).astype(F32)
        s, silu = silu_parts(g)
        down_s[n] += _dot(dy_t, (silu * u).astype(BF16), 1, 0)
        dg = (dact * u * (s + silu * (1 - s))).astype(BF16)
        du = (dact * silu).astype(BF16)
        gu_s[n] += _dot(b_t, dg, 1, 0)
        gu_s[3 + n] += _dot(b_t, du, 1, 0)
        db += _dot(dg, square(w, 2 + n), 1, 1) + _dot(du, square(w, 5 + n), 1, 1)
    dmid = (dy.astype(F32) + unit_back(wide, scale, db.astype(BF16).astype(F32))).astype(BF16)
    dmid_ref[...] = dmid
    dmid_t = dmid.T
    for m in range(2):
        o = jnp.concatenate([o_ref[4 * m + j] for j in range(4)], axis=1)
        o_s[m] += _dot(dmid_t, o, 1, 0)
        do = _dot(dmid, rows_o(w, m), 1, 1).astype(BF16)
        both = (do.astype(F32) * o.astype(F32)).T
        for j in range(4):
            do_ref[4 * m + j] = do[:, j * HEAD : (j + 1) * HEAD]
            delta_ref[2 * m + j // 2, j % 2 : j % 2 + 1, :] = both[j * HEAD : (j + 1) * HEAD].sum(0, keepdims=True)

    @pl.when(i == pl.num_programs(0) - 1)
    def _():
        for m in range(2):
            part = o_s[m].T.astype(BF16)
            for k in range(8):
                dw_ref[4 * m + k // 2, k % 2] = part[64 * k : 64 * k + 64]
        for n in range(6):
            dw_ref[:, 2 + n] = gu_s[n].astype(BF16).reshape(8, 64, D)
        for n in range(3):
            part = down_s[n].T.astype(BF16)
            for k in range(8):
                dw_ref[(8 * n + k) // 3, 8 + (8 * n + k) % 3] = part[64 * k : 64 * k + 64]


def mlp_back(states, dy, o, w, last, bt=512):
    t = dy.shape[0]
    specs, args = pieces(w)
    outs = [(tile(bt, D), shape((t, D))), (tile(8, bt, HEAD), shape((8, t, HEAD))),
            (pl.BlockSpec((4, 2, bt), lambda i: (0, 0, i)), shape((4, 2, t), F32)), grads(11)]
    return kernel_call(functools.partial(_mlp_back, last=last), t // bt, [tile(bt, D), tile(bt, D), tile(8, bt, HEAD)] + specs, outs,
                       [pltpu.VMEM((n, D, D), F32) for n in (6, 3, 2)], 2 * t * D * (15360 if last else 14336), [states, dy, o] + args)


def _qkv_back(h_ref, dq_ref, dk_ref, dv_ref, cos_ref, sin_ref, *refs, onward):
    if onward:
        dmid_ref, w, (dh_ref, dw_ref, acc_s) = refs[0], refs[1:5], refs[5:]
    else:
        dw_ref, acc_s = refs
    i = pl.program_id(0)

    @pl.when(i == 0)
    def _():
        acc_s[...] = jnp.zeros_like(acc_s)

    wide = h_ref[...].astype(F32)
    scale = unit(wide)
    a_t = (wide * scale).astype(BF16).T
    cos, sin = cos_ref[...], sin_ref[...]
    da = 0.0
    for n in range(4):
        parts = []
        for j in range(4):
            one = dq_ref[4 * n + j] if n < 2 else dk_ref[j] if n == 2 else dv_ref[j]
            if n < 3:
                f = one.astype(F32)
                one = (f * cos - pltpu.roll(f, HEAD // 2, 1) * sin).astype(BF16)
            parts.append(one)
        piece = jnp.concatenate(parts, axis=1)
        acc_s[n] += _dot(a_t, piece, 1, 0)
        if onward:
            da += _dot(piece, square(w, n), 1, 1)
    if onward:
        dh_ref[...] = (dmid_ref[...].astype(F32) + unit_back(wide, scale, da.astype(BF16).astype(F32))).astype(BF16)

    @pl.when(i == pl.num_programs(0) - 1)
    def _():
        for n in range(4):
            dw_ref[:, n] = acc_s[n].astype(BF16).reshape(8, 64, D)


def qkv_back(h, dq, dk, dv, cos, sin, dmid=None, w=None, bt=512):
    t = h.shape[0]
    onward = w is not None
    ins = [tile(bt, D)] + [tile(n, bt, HEAD) for n in (8, 4, 4)] + [tile(bt, HEAD)] * 2
    outs, args = [grads(4)], [h, dq, dk, dv, cos, sin]
    if onward:
        specs, more = pieces(w)
        ins += [tile(bt, D)] + specs
        outs = [(tile(bt, D), shape((t, D)))] + outs
        args += [dmid] + more
    return kernel_call(functools.partial(_qkv_back, onward=onward), t // bt, ins, outs, [pltpu.VMEM((4, D, D), F32)],
                       2 * t * D * (4096 if onward else 2048), args)


def adamw(w, m, v, g):
    m = 0.9 * m + 0.1 * g
    v = 0.95 * v + 0.05 * g * g
    step = m * lax.rsqrt(v + 1e-8) + 0.1 * w
    return (w - 0.02 * step).astype(jnp.bfloat16), m, v


def columns(w):
    return jnp.stack([w[:, at : at + D] for at in range(0, w.shape[1], D)])


def pack(*blocks):
    return jnp.concatenate([columns(w) if w.shape[0] == 64 else w.reshape(-1, 64, D) for w in blocks])


def unpack(a, b):
    side = lambda x: jnp.concatenate(list(x), axis=1)
    return side(a[0:2]), a[2], a[3], b[0:2].reshape(-1, D), side(b[2:5]), side(b[5:8]), b[8:11].reshape(-1, D)


def pairs(x):
    return x.reshape(4, 2, *x.shape[1:])


def solution(mesh):
    def step(x, dy, *arrays):
        weights, m, v = (arrays[i : i + 7] for i in (0, 7, 14))
        own = [[w[number] for w in weights] for number in range(2)]
        gather = lambda p: lax.all_gather(p, "dp", axis=0)
        scatter = lambda p: lax.psum_scatter(p, "dp", scatter_dimension=0)
        cos, sin = tables(x.shape[1])
        first = gather(pack(*own[0][:3]))
        second = gather(pack(*own[0][3:], *own[1][:3]))
        third = gather(pack(*own[1][3:]))
        a = [(first, 0, 4), (second, 11, 4)]
        b = [(second, 0, 11), (third, 0, 11)]
        h, kept = x[0], []
        for number in range(2):
            q, k, v_ = qkv(h, cos, sin, a[number])
            q = pairs(q)
            out, lse = attend(q, k, v_)
            o = out.reshape(8, *out.shape[2:])
            states = h
            if number == 0:
                states, y = mlp(h, o, b[number])
            kept.append((h, q, k, v_, o, lse, states))
            h = y
        g = dy[0]
        sums, held = [None, None], []
        for number in (1, 0):
            h, q, k, v_, o, lse, states = kept[number]
            dmid, do, delta, gb = mlp_back(states, g, o, b[number], number == 1)
            gb = scatter(gb)
            if held:
                do, held[0] = lax.optimization_barrier((do, held[0]))
            dq, dk, dv = attend_back(q, k, v_, pairs(do), lse, delta)
            dq, gb = lax.optimization_barrier((dq, gb))
            dq = dq.reshape(8, *dq.shape[2:])
            if number:
                g, ga = qkv_back(h, dq, dk, dv, cos, sin, dmid, a[number])
            else:
                (ga,) = qkv_back(h, dq, dk, dv, cos, sin)
            held.append(scatter(ga))
            sums[number] = gb
        gradients = [unpack(held[1 - number], sums[number]) for number in range(2)]
        gradients = [jnp.stack(pair).astype(F32) for pair in zip(*gradients, strict=True)]
        new = [adamw(w.astype(F32), m, v, g) for w, m, v, g in zip(weights, m, v, gradients, strict=True)]
        return tuple(one[which] for which in range(3) for one in new)

    states, cut = P(("rep", "dp"), None, None), P(None, "dp", None)
    return jax.shard_map(
        step,
        mesh=mesh,
        in_specs=(states, states) + (cut,) * 21,
        out_specs=(P("rep", "dp", None),) * 21,
        check_vma=False,
    )
```
